32 devices in a mesh: dp: 8 (over z, x), tp: 4 (over y, core).
Axes of the slice: x: 2, y: 2, z: 4, core: 2. Of those that a mesh axis runs over, the one named last changes fastest.
Arguments:
- gradients: bfloat16 [8, 4, 5120, 1280], P('dp', None, 'tp'), may hold values from -6 to 6
- right_factor: float32 [4, 1280, 32], replicated, may hold values from -6 to 6
- weights_before: float32 [4, 5120, 1280], P(None, 'tp', 'dp'), may hold values from -0.15625 to 0.15625
- momentum: float32 [4, 5120, 1280], P(None, 'tp', 'dp'), may hold values from -0.3125 to 0.3125
Outputs:
- new_weights: float32 [4, 5120, 1280], P(None, 'tp', 'dp')
- new_basis: float32 [4, 1280, 32], replicated
- new_momentum: float32 [4, 5120, 1280], P(None, 'tp', 'dp')
The draws below stay inside these ranges and needn't reach their ends.
All inputs are finite; a program needn't handle non-finite values.
Results may differ from the reference program's by a relative error of at most 0.003.
Values sent between devices are 32-bit elements; how exact they have to be, the bound alone decides.
A program may use at most 64 MiB of HBM per device.

```python
import jax
import jax.numpy as jnp
from jax import lax

WIDTH = 1280
INNER = 5120
RANK = 32
LAYERS = 4
REPLICAS = 8
N_TP = 4


def draw_gradients(key, part):
    keys = jax.random.split(key, 5)
    level = jnp.exp(jax.random.uniform(keys[4], (1, LAYERS, N_TP, 1, RANK), jnp.float32, -1.3, 1.3))
    left = jax.random.normal(keys[0], (1, LAYERS, N_TP, INNER // N_TP, RANK), jnp.float32) * level
    left = left.reshape(1, LAYERS, INNER, RANK)
    right = jax.random.normal(keys[1], (1, LAYERS, RANK, WIDTH), jnp.float32)
    strength = jax.random.normal(keys[2], (REPLICAS, LAYERS, 1, RANK), jnp.float32)
    noise = jax.random.normal(keys[3], (REPLICAS, LAYERS, INNER, WIDTH), jnp.float32)
    low = jnp.einsum('alir,lrw->aliw', left * strength, right[0])
    values = low * RANK ** (-0.5) + 0.5 * noise
    return jnp.clip(values, -6.0, 6.0).astype(jnp.bfloat16)


def block_levels(key, extent, cuts, least, largest):
    def one(position, blocks):
        steps = jax.random.uniform(jax.random.fold_in(jax.random.fold_in(key, 6), position), (blocks,), jnp.float32, least / len(cuts), largest / len(cuts))
        return jnp.repeat(jnp.exp(steps), extent[position] // blocks).reshape((-1,) + (1,) * (len(extent) - position - 1))

    gain = one(*cuts[0])
    for cut in cuts[1:]:
        gain = gain * one(*cut)
    return gain


def gaussian(stream_key, shape, scale, bound, cuts=(), held_as=jnp.bfloat16):
    values = jax.random.normal(stream_key, shape, jnp.float32) * scale
    if len(cuts) > 0:
        values = block_levels(stream_key, shape, cuts, -0.22, 0.18) * values
    return jnp.clip(values, min=-bound, max=bound).astype(held_as)


def setup_inputs(seed: int = 0) -> dict:
    arg_keys = jax.random.split(jax.random.key(seed), 5)
    gradients = draw_gradients(jax.random.fold_in(arg_keys[4], 71), 0)
    right_factor = gaussian(arg_keys[1], (LAYERS, WIDTH, RANK), 1.0, 6.0, (), jnp.float32)
    weights_before = gaussian(arg_keys[2], (LAYERS, INNER, WIDTH), WIDTH ** -0.5, 0.15625, ((1, 4), (2, 8)), jnp.float32)
    momentum = gaussian(arg_keys[3], (LAYERS, INNER, WIDTH), 0.05, 0.3125, ((1, 4), (2, 8)), jnp.float32)
    return {"gradients": gradients, "right_factor": right_factor, "weights_before": weights_before, "momentum": momentum}


def reference(gradients, right_factor, weights_before, momentum):
    small_basis = right_factor.astype(jnp.bfloat16)
    small_basis = lax.optimization_barrier(small_basis)
    left = jnp.einsum('aliw,lwr->lir', gradients.astype(jnp.float32), small_basis.astype(jnp.float32))
    gram = jnp.einsum('lir,lis->lrs', left, left, precision=lax.Precision.HIGHEST)
    gram = gram + 0.001 * lax.optimization_barrier(jnp.mean(jnp.diagonal(gram, axis1=1, axis2=2), axis=1))[:, None, None] * jnp.eye(RANK, dtype=jnp.float32)
    small_left = lax.optimization_barrier(left.astype(jnp.bfloat16))
    right = jnp.einsum('aliw,lir->lwr', gradients.astype(jnp.float32), small_left.astype(jnp.float32))
    root = jnp.linalg.cholesky(gram)
    half = lax.linalg.triangular_solve(root, jnp.swapaxes(right, 1, 2), left_side=True, lower=True)
    mixed = lax.linalg.triangular_solve(root, half, left_side=True, lower=True, transpose_a=True)
    change = jnp.einsum('lir,lrw->liw', left, mixed, precision=lax.Precision.HIGHEST) / REPLICAS
    new_momentum = 0.8 * momentum + change
    new_weights = weights_before - 0.05 * new_momentum
    new_basis = right * lax.rsqrt(lax.optimization_barrier(jnp.mean(right * right, axis=(1, 2), keepdims=True)) + 1e-12)
    return (new_weights, new_basis, new_momentum)
```

```python
import functools

import jax
import jax.numpy as jnp
from jax import lax
from jax.experimental import pallas as pl
from jax.experimental.pallas import tpu as pltpu
from jax.sharding import PartitionSpec as P

MESH = pl.DeviceIdType.MESH
HIGH = lax.Precision.HIGHEST
F32 = jnp.float32


def bits_of(n):
    count = n.bit_length() - 1
    assert 1 << count == n
    return count


def swapped_pairs(bits):
    out = list(bits)
    for at in range(0, len(out) - 1, 2):
        out[at], out[at + 1] = out[at + 1], out[at]
    return out


def cut(order, rows, unit=8):
    halved = []
    for bit in order:
        if rows % (2 * unit) == 0:
            halved.append(bit)
            rows //= 2
    return halved, rows


class Reduction:
    def __init__(self, order, dims, shape):
        self.dims = dims
        self.order = [b for b in order if b in dims] + [b for b in order if b not in dims]
        self.shape = shape
        self.full = (2,) * len(dims) + shape
        self.landing = []
        left = len(dims)
        for bit in self.order:
            if bit in dims:
                left -= 1
            self.landing.append((2,) * left + shape)
        self.copies = len(self.order) + len(dims)

    def scratch(self):
        return [pltpu.VMEM(s, F32) for s in [self.full, self.full if self.dims else self.shape] + self.landing]

    def run(self, refs, sems, first, places):
        work, total, landing = refs[0], refs[1], refs[2:]
        send_sem, recv_sem = sems
        slot = first

        def index(fixed, other=None):
            out = []
            for bit in self.dims:
                mine = places[bit][1]
                if bit == other:
                    out.append(1 - mine)
                elif bit in fixed:
                    out.append(mine)
                else:
                    out.append(slice(None))
            return tuple(out) + (slice(None),) * len(self.shape)

        def copy(src, dst, bit, slot):
            return pltpu.make_async_remote_copy(
                src_ref=src, dst_ref=dst, send_sem=send_sem.at[slot], recv_sem=recv_sem.at[slot],
                device_id=places[bit][0], device_id_type=MESH,
            )

        fixed = []
        for step, bit in enumerate(self.order):
            away = index(fixed, bit) if bit in self.dims else index(fixed)
            moving = copy(work.at[away], landing[step], bit, slot)
            slot += 1
            moving.start()
            yield
            moving.wait()
            if bit in self.dims:
                fixed.append(bit)
            own = index(fixed)
            into = total if step == len(self.order) - 1 else work
            into[own] = work[own] + landing[step][...]
        while fixed:
            own = index(fixed)
            bit = fixed.pop()
            moving = copy(total.at[own], total.at[own], bit, slot)
            slot += 1
            moving.start()
            yield
            moving.wait()


def advance(running):
    still = []
    for one in running:
        try:
            next(one)
            still.append(one)
        except StopIteration:
            pass
    return still


def factor_kernel(plan, g_hbm, qt_ref, lit_ref, right_ref, gv, qmask, left_t, right_t, g_sem, send_sem, recv_sem, *bufs):
    layers, rank, width = qt_ref.shape
    lanes = layers * rank
    n_dp, n_tp = plan["n_dp"], plan["n_tp"]
    piece, n_pieces = plan["piece"], plan["n_pieces"]
    me = {"dp": lax.axis_index("dp"), "tp": lax.axis_index("tp")}

    loads = []
    for p in range(n_pieces):
        rows = pl.ds(p * piece, piece)
        load = pltpu.make_async_copy(g_hbm.at[0, :, rows, :], gv.at[:, rows, :], g_sem.at[p])
        load.start()
        loads.append(load)

    places = {}
    for axis, n in (("dp", n_dp), ("tp", n_tp)):
        for b in range(bits_of(n)):
            bit = lax.rem(lax.div(me[axis], 1 << b), 2)
            partner = dict(me)
            partner[axis] = me[axis] + (1 - 2 * bit) * (1 << b)
            places[(axis, b)] = ((partner["dp"], partner["tp"]), bit)
    barrier = pltpu.get_barrier_semaphore()
    for target, _ in places.values():
        pl.semaphore_signal(barrier, inc=1, device_id=target, device_id_type=MESH)

    qt = qt_ref[...].reshape(lanes, width)
    owner = lax.broadcasted_iota(jnp.int32, (lanes, width), 0) // rank
    for l in range(layers):
        qmask[l] = jnp.where(owner == l, qt, 0.0).astype(jnp.bfloat16)
    pl.semaphore_wait(barrier, len(places))

    groups, at = [], 0
    for red in plan["reductions"]:
        count = 2 + len(red.landing)
        groups.append(bufs[at:at + count])
        at += count
    firsts, slot = [], 0
    for red in plan["reductions"]:
        firsts.append(slot)
        slot += red.copies

    def start(i):
        gen = plan["reductions"][i].run(groups[i], (send_sem, recv_sem), firsts[i], places)
        next(gen)
        return gen

    def absorb(p):
        rows = pl.ds(p * piece, piece)
        part = groups[p][1][...].reshape(piece, lanes).T
        left_t[:, rows] = part
        small = part.astype(jnp.bfloat16)
        for l in range(layers):
            out = pl.ds(l * rank, rank)
            term = jnp.dot(small[l * rank:(l + 1) * rank], gv[l, rows, :], preferred_element_type=F32)
            if p == 0:
                right_t[out, :] = term
            else:
                right_t[out, :] = right_t[out, :] + term

    def left_chain(p, gen):
        for _ in gen:
            yield
        absorb(p)

    running = []
    for p in range(n_pieces):
        loads[p].wait()
        rows = pl.ds(p * piece, piece)
        total = None
        for l in range(layers):
            term = lax.dot_general(
                gv[l, rows, :], qmask[l], (((1,), (1,)), ((), ())), preferred_element_type=F32
            )
            total = term if total is None else total + term
        groups[p][0][...] = total.reshape(plan["reductions"][p].full)
        running.append(left_chain(p, start(p)))
        if p >= 2:
            running[:p - 1] = advance(running[:p - 1])
    while running:
        running = advance(running)

    lay = lax.broadcasted_iota(jnp.int32, (layers, rank, lanes), 0)
    row = lax.broadcasted_iota(jnp.int32, (layers, rank, lanes), 1)
    lane = lax.broadcasted_iota(jnp.int32, (layers, rank, lanes), 2)
    block = lane // rank == lay

    def gram_chain():
        whole = left_t[...]
        gram = lax.dot_general(whole, whole, (((1,), (1,)), ((), ())), preferred_element_type=F32, precision=HIGH)
        packed = jnp.sum(jnp.where(block, gram.reshape(layers, rank, lanes), 0.0), axis=0)
        groups[n_pieces][0][...] = packed
        for _ in start_gram():
            yield
        b3 = jnp.where(block, groups[n_pieces][1][...][None], 0.0)
        diag = lane == lay * rank + row
        mean = jnp.sum(jnp.sum(jnp.where(diag, b3, 0.0), axis=1, keepdims=True), axis=2, keepdims=True) / rank
        b3 = jnp.where(diag, b3 + 0.001 * mean, b3)

        def sweep(k, b3):
            lane_k = lane == lay * rank + k
            row_k = row == k
            col = jnp.sum(jnp.where(lane_k, b3, 0.0), axis=2, keepdims=True)
            col = jnp.broadcast_to(col, b3.shape)
            pivot = jnp.sum(jnp.where(row_k, col, 0.0), axis=1, keepdims=True)
            line = jnp.sum(jnp.where(row_k, b3, 0.0), axis=1, keepdims=True)
            inv = 1.0 / pivot
            line = jnp.where(lane_k, inv, line * inv)
            return jnp.where(row_k, line, jnp.where(lane_k, 0.0, b3) - col * line)

        chunks = 4
        for c in range(chunks):
            lo, hi = c * rank // chunks, (c + 1) * rank // chunks
            b3 = lax.fori_loop(lo, hi, sweep, b3)
            yield
        inverse = b3.reshape(lanes, lanes)
        lit_ref[...] = jnp.dot(inverse, left_t[...], preferred_element_type=F32, precision=HIGH) * (1.0 / n_dp)

    def start_gram():
        yield from plan["reductions"][n_pieces].run(
            groups[n_pieces], (send_sem, recv_sem), firsts[n_pieces], places
        )

    gram = gram_chain()
    next(gram)
    running = []
    right = right_t[...].T.reshape((-1, plan["block"], lanes))
    at = 0
    for i, height in enumerate(plan["heights"]):
        k = n_pieces + 1 + i
        groups[k][0][...] = right[:, at:at + height, :].reshape(plan["reductions"][k].full)
        at += height
        running.append(start(k))
    running.append(gram)
    while running:
        running = advance(running)
    parts = []
    for i, height in enumerate(plan["heights"]):
        k = n_pieces + 1 + i
        parts.append(groups[k][1][...].reshape((-1, height, lanes)))
    at = 0
    for part, height in zip(parts, plan["heights"]):
        right_ref[:, at:at + height, :] = part
        at += height


def update_kernel(lit_ref, right_ref, w_ref, m_ref, nw_ref, nb_ref, nm_ref, right_t):
    l = pl.program_id(0)
    own = w_ref.shape[1]
    rank = nb_ref.shape[1]
    width, lanes = right_ref.shape

    @pl.when(l == 0)
    def _():
        right_t[...] = right_ref[...].T

    mine = right_ref[pl.ds(pl.multiple_of(lax.axis_index("dp") * own, 8), own), :]
    lane = lax.broadcasted_iota(jnp.int32, (own, lanes), 1)
    mine = jnp.where(lane // rank == l, mine, 0.0)
    change = jnp.dot(mine, lit_ref[...], preferred_element_type=F32, precision=HIGH)
    momentum = 0.8 * m_ref[0] + change
    nm_ref[0] = momentum
    nw_ref[0] = w_ref[0] - 0.05 * momentum
    basis = right_t[pl.ds(pl.multiple_of(l * rank, 8), rank), :]
    mean = jnp.sum(jnp.sum(basis * basis, axis=1, keepdims=True), axis=0, keepdims=True) / (width * rank)
    nb_ref[0] = basis * lax.rsqrt(mean + 1e-12)


def make_plan(n_dp, n_tp, rows, width, lanes, rank):
    dp = [("dp", b) for b in range(bits_of(n_dp))]
    tp = [("tp", b) for b in range(bits_of(n_tp))]
    piece = 256 if rows % 256 == 0 else rows
    n_pieces = rows // piece
    reductions = []
    for p in range(n_pieces):
        order = dp if p % 2 == 0 else swapped_pairs(dp)
        dims, height = cut(order, piece)
        reductions.append(Reduction(order, sorted(dims, reverse=True), (height, lanes)))
    reductions.append(Reduction(tp, [], (rank, lanes)))
    per = width // n_dp
    dims, block = cut(tp, per)
    tiles = block // 8
    heights = [block] if tiles < 2 else [(tiles + 1) // 2 * 8, tiles // 2 * 8]
    dims = sorted(dp, reverse=True) + sorted(dims, reverse=True)
    for i, height in enumerate(heights):
        order = tp + dp if i % 2 == 0 else swapped_pairs(tp) + swapped_pairs(dp)
        reductions.append(Reduction(order, dims, (height, lanes)))
    return dict(
        n_dp=n_dp, n_tp=n_tp, piece=piece, n_pieces=n_pieces, reductions=reductions, heights=heights, block=block,
        copies=sum(r.copies for r in reductions),
    )


def solution(mesh):
    n_dp, n_tp = mesh.shape["dp"], mesh.shape["tp"]

    def on_device(gradients, right_factor, weights_before, momentum):
        _, layers, rows, width = gradients.shape
        rank = right_factor.shape[2]
        lanes = layers * rank
        own = weights_before.shape[2]
        plan = make_plan(n_dp, n_tp, rows, width, lanes, rank)
        vmem = pl.BlockSpec(memory_space=pltpu.VMEM)
        scratch = [
            pltpu.VMEM((layers, rows, width), jnp.bfloat16),
            pltpu.VMEM((layers, lanes, width), jnp.bfloat16),
            pltpu.VMEM((lanes, rows), F32),
            pltpu.VMEM((lanes, width), F32),
            pltpu.SemaphoreType.DMA((plan["n_pieces"],)),
            pltpu.SemaphoreType.DMA((plan["copies"],)),
            pltpu.SemaphoreType.DMA((plan["copies"],)),
        ]
        for red in plan["reductions"]:
            scratch += red.scratch()
        lit, right = pl.pallas_call(
            functools.partial(factor_kernel, plan),
            out_shape=(
                jax.ShapeDtypeStruct((lanes, rows), F32),
                jax.ShapeDtypeStruct((width // plan["block"], plan["block"], lanes), F32),
            ),
            in_specs=[pl.BlockSpec(memory_space=pl.ANY), vmem],
            out_specs=(vmem, vmem),
            scratch_shapes=scratch,
            compiler_params=pltpu.CompilerParams(
                collective_id=0, has_side_effects=True, vmem_limit_bytes=40 * 1024 * 1024
            ),
            name="factors",
        )(gradients, jnp.swapaxes(right_factor, 1, 2))
        right = right.reshape(width, lanes)
        one = lambda a, b: pl.BlockSpec((1, a, b), lambda l: (l, 0, 0))
        whole = lambda a, b: pl.BlockSpec((a, b), lambda l: (0, 0))
        new_w, new_b, new_m = pl.pallas_call(
            update_kernel,
            grid=(layers,),
            out_shape=(
                jax.ShapeDtypeStruct((layers, own, rows), F32),
                jax.ShapeDtypeStruct((layers, rank, width), F32),
                jax.ShapeDtypeStruct((layers, own, rows), F32),
            ),
            in_specs=[whole(lanes, rows), whole(width, lanes), one(own, rows), one(own, rows)],
            out_specs=(one(own, rows), one(rank, width), one(own, rows)),
            scratch_shapes=[pltpu.VMEM((lanes, width), F32)],
            compiler_params=pltpu.CompilerParams(dimension_semantics=("arbitrary",)),
            name="update",
        )(lit, right, jnp.swapaxes(weights_before, 1, 2), jnp.swapaxes(momentum, 1, 2))
        return tuple(jnp.swapaxes(a, 1, 2) for a in (new_w, new_b, new_m))

    return jax.shard_map(
        on_device,
        mesh=mesh,
        in_specs=(P("dp", None, "tp", None), P(), P(None, "tp", "dp"), P(None, "tp", "dp")),
        out_specs=(P(None, "tp", "dp"), P(), P(None, "tp", "dp")),
        check_vma=False,
    )
```

```python
import functools

import jax
import jax.numpy as jnp
from jax import lax
from jax.experimental import pallas as pl
from jax.experimental.pallas import tpu as pltpu
from jax.sharding import PartitionSpec as P

MESH = pl.DeviceIdType.MESH
HIGH = lax.Precision.HIGHEST
F32 = jnp.float32


def bits_of(n):
    count = n.bit_length() - 1
    assert 1 << count == n
    return count


def swapped_pairs(bits):
    out = list(bits)
    for at in range(0, len(out) - 1, 2):
        out[at], out[at + 1] = out[at + 1], out[at]
    return out


def cut(order, rows, unit=8):
    halved = []
    for bit in order:
        if rows % (2 * unit) == 0:
            halved.append(bit)
            rows //= 2
    return halved, rows


class Reduction:
    def __init__(self, order, dims, shape):
        self.dims = dims
        self.order = [b for b in order if b in dims] + [b for b in order if b not in dims]
        self.shape = shape
        self.full = (2,) * len(dims) + shape
        self.landing = []
        left = len(dims)
        for bit in self.order:
            if bit in dims:
                left -= 1
            self.landing.append((2,) * left + shape)
        self.copies = len(self.order) + len(dims)

    def scratch(self):
        return [pltpu.VMEM(s, F32) for s in [self.full, self.full if self.dims else self.shape] + self.landing]

    def run(self, refs, sems, first, places):
        work, total, landing = refs[0], refs[1], refs[2:]
        send_sem, recv_sem = sems
        slot = first

        def index(fixed, other=None):
            out = []
            for bit in self.dims:
                mine = places[bit][1]
                if bit == other:
                    out.append(1 - mine)
                elif bit in fixed:
                    out.append(mine)
                else:
                    out.append(slice(None))
            return tuple(out) + (slice(None),) * len(self.shape)

        def copy(src, dst, bit, slot):
            return pltpu.make_async_remote_copy(
                src_ref=src, dst_ref=dst, send_sem=send_sem.at[slot], recv_sem=recv_sem.at[slot],
                device_id=places[bit][0], device_id_type=MESH,
            )

        fixed = []
        for step, bit in enumerate(self.order):
            away = index(fixed, bit) if bit in self.dims else index(fixed)
            moving = copy(work.at[away], landing[step], bit, slot)
            slot += 1
            moving.start()
            yield
            moving.wait()
            if bit in self.dims:
                fixed.append(bit)
            own = index(fixed)
            into = total if step == len(self.order) - 1 else work
            into[own] = work[own] + landing[step][...]
        while fixed:
            own = index(fixed)
            bit = fixed.pop()
            moving = copy(total.at[own], total.at[own], bit, slot)
            slot += 1
            moving.start()
            yield
            moving.wait()


def advance(running):
    still = []
    for one in running:
        try:
            next(one)
            still.append(one)
        except StopIteration:
            pass
    return still


def factor_kernel(plan, g_hbm, qt_ref, lit_ref, right_ref, gv, qmask, left_t, right_t, g_sem, send_sem, recv_sem, *bufs):
    layers, rank, width = qt_ref.shape
    lanes = layers * rank
    n_dp, n_tp = plan["n_dp"], plan["n_tp"]
    piece, n_pieces = plan["piece"], plan["n_pieces"]
    me = {"dp": lax.axis_index("dp"), "tp": lax.axis_index("tp")}

    loads = []
    for p in range(n_pieces):
        rows = pl.ds(p * piece, piece)
        load = pltpu.make_async_copy(g_hbm.at[0, :, rows, :], gv.at[:, rows, :], g_sem.at[p])
        load.start()
        loads.append(load)

    places = {}
    for axis, n in (("dp", n_dp), ("tp", n_tp)):
        for b in range(bits_of(n)):
            bit = lax.rem(lax.div(me[axis], 1 << b), 2)
            partner = dict(me)
            partner[axis] = me[axis] + (1 - 2 * bit) * (1 << b)
            places[(axis, b)] = ((partner["dp"], partner["tp"]), bit)
    barrier = pltpu.get_barrier_semaphore()
    for target, _ in places.values():
        pl.semaphore_signal(barrier, inc=1, device_id=target, device_id_type=MESH)

    q = qt_ref[...].reshape(lanes, width).T
    owner = lax.broadcasted_iota(jnp.int32, (width, lanes), 1) // rank
    for l in range(layers):
        qmask[l] = jnp.where(owner == l, q, 0.0).astype(jnp.bfloat16)
    pl.semaphore_wait(barrier, len(places))

    groups, at = [], 0
    for red in plan["reductions"]:
        count = 2 + len(red.landing)
        groups.append(bufs[at:at + count])
        at += count
    firsts, slot = [], 0
    for red in plan["reductions"]:
        firsts.append(slot)
        slot += red.copies

    def start(i):
        gen = plan["reductions"][i].run(groups[i], (send_sem, recv_sem), firsts[i], places)
        next(gen)
        return gen

    def absorb(p):
        rows = pl.ds(p * piece, piece)
        part = groups[p][1][...].reshape(piece, lanes).T
        left_t[:, rows] = part
        small = part.astype(jnp.bfloat16)
        for l in range(layers):
            out = pl.ds(l * rank, rank)
            term = jnp.dot(small[l * rank:(l + 1) * rank], gv[l, rows, :], preferred_element_type=F32)
            if p == 0:
                right_t[out, :] = term
            else:
                right_t[out, :] = right_t[out, :] + term

    def left_chain(p, gen):
        for _ in gen:
            yield
        absorb(p)

    running = []
    for p in range(n_pieces):
        loads[p].wait()
        rows = pl.ds(p * piece, piece)
        total = None
        for l in range(layers):
            term = jnp.dot(gv[l, rows, :], qmask[l], preferred_element_type=F32)
            total = term if total is None else total + term
        groups[p][0][...] = total.reshape(plan["reductions"][p].full)
        running.append(left_chain(p, start(p)))
        if p >= 2:
            running[:p - 1] = advance(running[:p - 1])
    while running:
        running = advance(running)

    lay = lax.broadcasted_iota(jnp.int32, (layers, rank, lanes), 0)
    row = lax.broadcasted_iota(jnp.int32, (layers, rank, lanes), 1)
    lane = lax.broadcasted_iota(jnp.int32, (layers, rank, lanes), 2)
    block = lane // rank == lay

    def gram_chain():
        whole = left_t[...]
        gram = lax.dot_general(whole, whole, (((1,), (1,)), ((), ())), preferred_element_type=F32, precision=HIGH)
        packed = jnp.sum(jnp.where(block, gram.reshape(layers, rank, lanes), 0.0), axis=0)
        groups[n_pieces][0][...] = packed
        for _ in start_gram():
            yield
        b3 = jnp.where(block, groups[n_pieces][1][...][None], 0.0)
        diag = lane == lay * rank + row
        mean = jnp.sum(jnp.sum(jnp.where(diag, b3, 0.0), axis=1, keepdims=True), axis=2, keepdims=True) / rank
        b3 = jnp.where(diag, b3 + 0.001 * mean, b3)

        def sweep(k, b3):
            lane_k = lane == lay * rank + k
            row_k = row == k
            col = jnp.sum(jnp.where(lane_k, b3, 0.0), axis=2, keepdims=True)
            col = jnp.broadcast_to(col, b3.shape)
            pivot = jnp.sum(jnp.where(row_k, col, 0.0), axis=1, keepdims=True)
            line = jnp.sum(jnp.where(row_k, b3, 0.0), axis=1, keepdims=True)
            inv = 1.0 / pivot
            line = jnp.where(lane_k, inv, line * inv)
            return jnp.where(row_k, line, jnp.where(lane_k, 0.0, b3) - col * line)

        chunks = 4
        for c in range(chunks):
            lo, hi = c * rank // chunks, (c + 1) * rank // chunks
            b3 = lax.fori_loop(lo, hi, sweep, b3)
            yield
        inverse = b3.reshape(lanes, lanes)
        lit_ref[...] = jnp.dot(inverse, left_t[...], preferred_element_type=F32, precision=HIGH) * (1.0 / n_dp)

    def start_gram():
        yield from plan["reductions"][n_pieces].run(
            groups[n_pieces], (send_sem, recv_sem), firsts[n_pieces], places
        )

    running = []
    right = right_t[...].T.reshape((-1, plan["block"], lanes))
    at = 0
    for i, height in enumerate(plan["heights"]):
        k = n_pieces + 1 + i
        groups[k][0][...] = right[:, at:at + height, :].reshape(plan["reductions"][k].full)
        at += height
        running.append(start(k))
    running += advance([gram_chain()])
    while running:
        running = advance(running)
    parts = []
    for i, height in enumerate(plan["heights"]):
        k = n_pieces + 1 + i
        parts.append(groups[k][1][...].reshape((-1, height, lanes)))
    at = 0
    for part, height in zip(parts, plan["heights"]):
        right_ref[:, at:at + height, :] = part
        at += height


def update_kernel(lit_ref, right_ref, w_ref, m_ref, nw_ref, nb_ref, nm_ref, right_t):
    l = pl.program_id(0)
    own = w_ref.shape[1]
    rank = nb_ref.shape[1]
    width, lanes = right_ref.shape

    @pl.when(l == 0)
    def _():
        right_t[...] = right_ref[...].T

    mine = right_ref[pl.ds(pl.multiple_of(lax.axis_index("dp") * own, 8), own), :]
    lane = lax.broadcasted_iota(jnp.int32, (own, lanes), 1)
    mine = jnp.where(lane // rank == l, mine, 0.0)
    change = jnp.dot(mine, lit_ref[...], preferred_element_type=F32, precision=HIGH)
    momentum = 0.8 * m_ref[0] + change
    nm_ref[0] = momentum
    nw_ref[0] = w_ref[0] - 0.05 * momentum
    basis = right_t[pl.ds(pl.multiple_of(l * rank, 8), rank), :]
    mean = jnp.sum(jnp.sum(basis * basis, axis=1, keepdims=True), axis=0, keepdims=True) / (width * rank)
    nb_ref[0] = basis * lax.rsqrt(mean + 1e-12)


def make_plan(n_dp, n_tp, rows, width, lanes, rank):
    dp = [("dp", b) for b in range(bits_of(n_dp))]
    tp = [("tp", b) for b in range(bits_of(n_tp))]
    piece = rows // 2 if rows % 256 == 0 else rows
    n_pieces = rows // piece
    reductions = []
    for p in range(n_pieces):
        order = dp if p % 2 == 0 else swapped_pairs(dp)
        dims, height = cut(order, piece)
        reductions.append(Reduction(order, sorted(dims, reverse=True), (height, lanes)))
    reductions.append(Reduction(tp, [], (rank, lanes)))
    per = width // n_dp
    dims, block = cut(tp, per)
    tiles = block // 8
    heights = [block] if tiles < 2 else [(tiles + 1) // 2 * 8, tiles // 2 * 8]
    dims = sorted(dp, reverse=True) + sorted(dims, reverse=True)
    for i, height in enumerate(heights):
        order = tp + dp if i % 2 == 0 else swapped_pairs(tp) + swapped_pairs(dp)
        reductions.append(Reduction(order, dims, (height, lanes)))
    return dict(
        n_dp=n_dp, n_tp=n_tp, piece=piece, n_pieces=n_pieces, reductions=reductions, heights=heights, block=block,
        copies=sum(r.copies for r in reductions),
    )


def solution(mesh):
    n_dp, n_tp = mesh.shape["dp"], mesh.shape["tp"]

    def on_device(gradients, right_factor, weights_before, momentum):
        _, layers, rows, width = gradients.shape
        rank = right_factor.shape[2]
        lanes = layers * rank
        own = weights_before.shape[2]
        plan = make_plan(n_dp, n_tp, rows, width, lanes, rank)
        vmem = pl.BlockSpec(memory_space=pltpu.VMEM)
        scratch = [
            pltpu.VMEM((layers, rows, width), jnp.bfloat16),
            pltpu.VMEM((layers, width, lanes), jnp.bfloat16),
            pltpu.VMEM((lanes, rows), F32),
            pltpu.VMEM((lanes, width), F32),
            pltpu.SemaphoreType.DMA((plan["n_pieces"],)),
            pltpu.SemaphoreType.DMA((plan["copies"],)),
            pltpu.SemaphoreType.DMA((plan["copies"],)),
        ]
        for red in plan["reductions"]:
            scratch += red.scratch()
        lit, right = pl.pallas_call(
            functools.partial(factor_kernel, plan),
            out_shape=(
                jax.ShapeDtypeStruct((lanes, rows), F32),
                jax.ShapeDtypeStruct((width // plan["block"], plan["block"], lanes), F32),
            ),
            in_specs=[pl.BlockSpec(memory_space=pl.ANY), vmem],
            out_specs=(vmem, vmem),
            scratch_shapes=scratch,
            compiler_params=pltpu.CompilerParams(
                collective_id=0, has_side_effects=True, vmem_limit_bytes=40 * 1024 * 1024
            ),
            name="factors",
        )(gradients, jnp.swapaxes(right_factor, 1, 2))
        right = right.reshape(width, lanes)
        one = lambda a, b: pl.BlockSpec((1, a, b), lambda l: (l, 0, 0))
        whole = lambda a, b: pl.BlockSpec((a, b), lambda l: (0, 0))
        new_w, new_b, new_m = pl.pallas_call(
            update_kernel,
            grid=(layers,),
            out_shape=(
                jax.ShapeDtypeStruct((layers, own, rows), F32),
                jax.ShapeDtypeStruct((layers, rank, width), F32),
                jax.ShapeDtypeStruct((layers, own, rows), F32),
            ),
            in_specs=[whole(lanes, rows), whole(width, lanes), one(own, rows), one(own, rows)],
            out_specs=(one(own, rows), one(rank, width), one(own, rows)),
            scratch_shapes=[pltpu.VMEM((lanes, width), F32)],
            compiler_params=pltpu.CompilerParams(
                dimension_semantics=("arbitrary",), vmem_limit_bytes=20 * 1024 * 1024
            ),
            name="update",
        )(lit, right, jnp.swapaxes(weights_before, 1, 2), jnp.swapaxes(momentum, 1, 2))
        return tuple(jnp.swapaxes(a, 1, 2) for a in (new_w, new_b, new_m))

    return jax.shard_map(
        on_device,
        mesh=mesh,
        in_specs=(P("dp", None, "tp", None), P(), P(None, "tp", "dp"), P(None, "tp", "dp")),
        out_specs=(P(None, "tp", "dp"), P(), P(None, "tp", "dp")),
        check_vma=False,
    )
```
